32 devices in a mesh: agent: 4 (over x, core), tp: 8 (over z, y).
Axes of the slice: x: 2, y: 2, z: 4, core: 2. Of those that a mesh axis runs over, the one named last changes fastest.
Arguments:
- tokens: bfloat16 [4, 512, 2048], P('agent', 'tp'), may hold values from -6 to 6
- targets: bfloat16 [4, 512, 2048], P('agent', 'tp'), may hold values from -6 to 6
- params: bfloat16 [4, 2048, 8192], P('agent', None, 'tp'), may hold values from -6 to 6
- tracker: bfloat16 [4, 2048, 8192], P('agent', None, 'tp'), may hold values from -6 to 6
- up_weight: bfloat16 [2048, 8192], P('agent', 'tp'), may hold values from -0.125 to 0.125
- down_weight: bfloat16 [8192, 2048], P('tp', 'agent'), may hold values from -0.0625 to 0.0625
- edge_weight: float32 [4], replicated, may hold values from 0.1 to 0.4
- step_size: float32 [1], replicated, may hold values from 0.1 to 0.5
Outputs:
- new_params: bfloat16 [4, 2048, 8192], P('agent', None, 'tp')
- new_tracker: bfloat16 [4, 2048, 8192], P('agent', None, 'tp')
The draws below stay inside these ranges and needn't reach their ends.
All inputs are finite; a program needn't handle non-finite values.
Results may differ from the reference program's by a relative error of at most 0.033.
Values may be sent and summed in bfloat16 or wider, within the bound.
No kernel may reach another device: no remote copies, remote signals or barrier semaphores. Data moves between devices by JAX's collectives and lax.ppermute only.
A program may use at most 128 MiB of HBM per device.

```python
import math
import jax
import jax.numpy as jnp
from jax import lax

D = 2048
FF = 8192
TOKENS = 512
AGENTS = 4
N_TP = 8


def shard_levels(key, dims, cuts, least, top_value):
    def one(position, parts):
        heights = jax.random.uniform(jax.random.fold_in(jax.random.fold_in(key, 6), position), (parts,), jnp.float32, least / len(cuts), top_value / len(cuts))
        return jnp.repeat(jnp.exp(heights), dims[position] // parts).reshape((-1,) + (1,) * (len(dims) - position - 1))

    factor_of = one(*cuts[0])
    for cut in cuts[1:]:
        factor_of = factor_of * one(*cut)
    return factor_of


def normal_values(rng, shape, deviation, bound, cuts=(), dtype=jnp.bfloat16):
    entries = deviation * jax.random.normal(rng, shape, jnp.float32)
    if cuts:
        entries = entries * shard_levels(rng, shape, cuts, -0.22, 0.18)
    return jnp.clip(entries, -bound, bound).astype(dtype)


def setup_inputs(seed: int = 0) -> dict:
    keys = jax.random.split(jax.random.key(seed), 9)
    return {
        "tokens": normal_values(keys[0], (AGENTS, TOKENS, D), 1.0, 6.0, ((0, 4), (1, 8))),
        "targets": normal_values(keys[1], (AGENTS, TOKENS, D), 1.0, 6.0, ((0, 4), (1, 8))),
        "params": normal_values(keys[2], (AGENTS, D, FF), 1.0, 6.0, ((0, 4), (2, 8))),
        "tracker": normal_values(keys[3], (AGENTS, D, FF), 1.0, 6.0, ((0, 4), (2, 8))),
        "up_weight": normal_values(keys[4], (D, FF), D ** -0.5, 0.125, ((0, 4), (1, 8))),
        "down_weight": normal_values(keys[5], (FF, D), FF ** -0.5, 0.0625, ((0, 8), (1, 4))),
        "edge_weight": jnp.clip(jax.random.uniform(keys[6], (AGENTS,), jnp.float32, 0.1, 0.4), 0.1, 0.4),
        "step_size": jnp.clip(jnp.exp(jax.random.uniform(keys[7], (1,), jnp.float32, math.log(0.1), math.log(0.5))), 0.1, 0.5),
    }


def gate_grad(tok, param, up_weight, down_weight, target):
    scale = 1.0 / D ** 0.5
    gate = jnp.dot(tok, param, preferred_element_type=jnp.float32) * scale
    up = jnp.dot(tok, up_weight, preferred_element_type=jnp.float32)
    hidden = (jax.nn.sigmoid(gate) * gate * up).astype(jnp.bfloat16)
    group = FF // N_TP
    hidden_groups = hidden.reshape(hidden.shape[0], N_TP, group).transpose(1, 0, 2)
    down_groups = down_weight.reshape(N_TP, group, down_weight.shape[1])

    def add_share(total, items):
        piece, weights = items
        share = jnp.dot(piece, weights, preferred_element_type=jnp.float32).astype(jnp.bfloat16)
        return (total + share.astype(jnp.float32), None)
    start = jnp.zeros((hidden.shape[0], down_weight.shape[1]), jnp.float32)
    out, unused = lax.scan(add_share, start, (hidden_groups, down_groups))
    err = (2.0 * (out - target.astype(jnp.float32))).astype(jnp.bfloat16)
    back = jnp.dot(err, down_weight.T, preferred_element_type=jnp.float32)
    sig = jax.nn.sigmoid(gate)
    dgate = (back * up * sig * (1.0 + gate * (1.0 - sig))).astype(jnp.bfloat16)
    return jnp.dot(tok.T, dgate, preferred_element_type=jnp.float32) * scale

def reference(tokens, targets, params, tracker, up_weight, down_weight, edge_weight, step_size):
    params32 = params.astype(jnp.float32)
    tracker32 = tracker.astype(jnp.float32)
    e_right = edge_weight
    e_left = jnp.roll(edge_weight, 1)
    own = 1.0 - e_right - e_left
    e_right = e_right[:, None, None]
    e_left = e_left[:, None, None]
    own = own[:, None, None]
    mixed_x = own * params32 + e_right * jnp.roll(params32, -1, axis=0) + e_left * jnp.roll(params32, 1, axis=0)
    mixed_y = own * tracker32 + e_right * jnp.roll(tracker32, -1, axis=0) + e_left * jnp.roll(tracker32, 1, axis=0)
    new_params = (mixed_x - step_size[0] * tracker32).astype(jnp.bfloat16)

    def one_agent(items):
        tok, target, param, fresh = items
        before = gate_grad(tok, param, up_weight, down_weight, target)
        after = gate_grad(tok, fresh, up_weight, down_weight, target)
        return after - before
    change = lax.map(one_agent, (tokens, targets, params, new_params))
    new_tracker = (mixed_y + change).astype(jnp.bfloat16)
    return (new_params, new_tracker)
```

```python
import functools

import jax
import jax.numpy as jnp
from jax import lax
from jax.experimental import pallas as pl
from jax.experimental.pallas import tpu as pltpu
from jax.sharding import PartitionSpec as P


F32 = jnp.float32
BF16 = jnp.bfloat16
CHUNKS = 4


def shifted(value, axis, shift):
    count = lax.axis_size(axis)
    return lax.ppermute(value, axis, [(source, (source + shift) % count) for source in range(count)])


def paired(value, axis):
    return lax.ppermute(value, axis, [(source, source ^ 1) for source in range(lax.axis_size(axis))])


def jumped(value, axis, shift):
    return shifted(value, axis, 2 * shift)


def cost(flops, *arrays):
    return pl.CostEstimate(
        flops=flops, bytes_accessed=sum(a.size * a.dtype.itemsize for a in arrays), transcendentals=0
    )


def block_of(size, most):
    return most if size % most == 0 else size


def gate_kernel(scale, tok_ref, w_ref, out_ref):
    out_ref[...] = jnp.dot(tok_ref[...], w_ref[...], preferred_element_type=F32) * scale


def gate_of(tok, weights, scale):
    rows, depth = tok.shape
    width = weights.shape[1]
    cols = block_of(width, 256)
    out = jax.ShapeDtypeStruct((rows, width), F32)
    return pl.pallas_call(
        functools.partial(gate_kernel, scale),
        grid=(width // cols,),
        in_specs=[
            pl.BlockSpec((rows, depth), lambda i: (0, 0)),
            pl.BlockSpec((depth, cols), lambda i: (0, i)),
        ],
        out_specs=pl.BlockSpec((rows, cols), lambda i: (0, i)),
        out_shape=out,
        cost_estimate=cost(2 * rows * depth * width, tok, weights, out),
        name="gate",
    )(tok, weights)


def chip_index(place, j, half):
    return lax.rem(place[0] - j + half, half)


def up_kernel(place, tok_ref, own_ref, other_ref, out_ref):
    j = pl.program_id(0)
    depth = own_ref.shape[0]

    @pl.when(j == 0)
    def _():
        out_ref[...] = jnp.zeros_like(out_ref)

    def add(first, second):
        out_ref[...] += jnp.dot(tok_ref[:, :depth], first[...], preferred_element_type=F32) + jnp.dot(
            tok_ref[:, depth:], second[...], preferred_element_type=F32
        )

    @pl.when(place[1] == 0)
    def _():
        add(own_ref, other_ref)

    @pl.when(place[1] != 0)
    def _():
        add(other_ref, own_ref)


def up_of(place, tok, own, other):
    half, depth, width = own.shape
    rows = tok.shape[0]
    out = jax.ShapeDtypeStruct((rows, width), F32)
    piece = pl.BlockSpec((None, depth, width), lambda j, place: (j, 0, 0))
    return pl.pallas_call(
        up_kernel,
        grid_spec=pltpu.PrefetchScalarGridSpec(
            num_scalar_prefetch=1,
            grid=(half,),
            in_specs=[
                pl.BlockSpec((rows, 2 * depth), lambda j, place: (0, chip_index(place, j, half))),
                piece,
                piece,
            ],
            out_specs=pl.BlockSpec((rows, width), lambda j, place: (0, 0)),
        ),
        out_shape=out,
        cost_estimate=cost(4 * rows * half * depth * width, tok, own, other, out),
        name="up",
    )(place, tok, own, other)


def share_kernel(place, gate_ref, up_ref, own_ref, other_ref, *rest):
    near_ref, far_refs, hidden = rest[0], rest[1:-1], rest[-1]
    cols = own_ref.shape[1]
    near = near_ref.shape[0]
    piece = far_refs[0].shape[0]

    @pl.when(pl.program_id(0) == 0)
    def _():
        gate = gate_ref[...]
        hidden[...] = (jax.nn.sigmoid(gate) * gate * up_ref[...]).astype(BF16)

    def fill(first, second):
        for at, ref in ((0, first), (cols, second)):
            share = jnp.dot(hidden[...], ref[...], preferred_element_type=F32).astype(BF16)
            near_ref[:, at : at + cols] = share[:near]
            for k, far_ref in enumerate(far_refs):
                start = near + k * piece
                far_ref[:, at : at + cols] = share[start : start + piece]

    @pl.when(place[1] == 0)
    def _():
        fill(own_ref, other_ref)

    @pl.when(place[1] != 0)
    def _():
        fill(other_ref, own_ref)


def share_of(place, gate, up, own, other, pieces):
    half, width, cols = own.shape
    rows = gate.shape[0]
    near, piece = rows // 2, rows // 2 // pieces
    weights = pl.BlockSpec((None, width, cols), lambda j, place: (j, 0, 0))
    whole = pl.BlockSpec((rows, width), lambda j, place: (0, 0))
    depth = 2 * cols * half
    out = [jax.ShapeDtypeStruct((near, depth), BF16)] + [
        jax.ShapeDtypeStruct((piece, depth), BF16) for _ in range(pieces)
    ]
    return pl.pallas_call(
        share_kernel,
        grid_spec=pltpu.PrefetchScalarGridSpec(
            num_scalar_prefetch=1,
            grid=(half,),
            in_specs=[whole, whole, weights, weights],
            out_specs=[
                pl.BlockSpec((o.shape[0], 2 * cols), lambda j, place: (0, chip_index(place, j, half)))
                for o in out
            ],
            scratch_shapes=[pltpu.VMEM((rows, width), BF16)],
        ),
        out_shape=out,
        cost_estimate=cost(2 * rows * width * depth, gate, up, own, other, *out),
        name="share",
    )(place, gate, up, own, other)


def back_kernel(count, place, gate_ref, up_ref, own_ref, other_ref, *rest):
    pieces, out_ref, err, total = rest[:count], rest[count], rest[count + 1], rest[count + 2]
    j = pl.program_id(0)
    cols = own_ref.shape[1]
    piece = pieces[0].shape[0]

    @pl.when(j == 0)
    def _():
        total[...] = jnp.zeros_like(total)

    for k, ref in enumerate(pieces):
        err[k * piece : (k + 1) * piece, :] = ref[...]

    def add(first, second):
        dims = (((1,), (1,)), ((), ()))
        total[...] += lax.dot_general(
            err[:, :cols], first[...], dims, preferred_element_type=F32
        ) + lax.dot_general(err[:, cols:], second[...], dims, preferred_element_type=F32)

    @pl.when(place[1] == 0)
    def _():
        add(own_ref, other_ref)

    @pl.when(place[1] != 0)
    def _():
        add(other_ref, own_ref)

    @pl.when(j == pl.num_programs(0) - 1)
    def _():
        gate = gate_ref[...]
        sig = jax.nn.sigmoid(gate)
        out_ref[...] = (total[...] * up_ref[...] * sig * (1.0 + gate * (1.0 - sig))).astype(BF16)


def dgate_of(place, gate, up, own, other, pieces):
    half, width, cols = own.shape
    rows = gate.shape[0]
    piece = pieces[0].shape[0]
    weights = pl.BlockSpec((None, width, cols), lambda j, place: (j, 0, 0))
    whole = pl.BlockSpec((rows, width), lambda j, place: (0, 0))
    out = jax.ShapeDtypeStruct((rows, width), BF16)
    return pl.pallas_call(
        functools.partial(back_kernel, len(pieces)),
        grid_spec=pltpu.PrefetchScalarGridSpec(
            num_scalar_prefetch=1,
            grid=(half,),
            in_specs=[whole, whole, weights, weights]
            + [pl.BlockSpec((piece, 2 * cols), lambda j, place: (0, chip_index(place, j, half)))] * len(pieces),
            out_specs=whole,
            scratch_shapes=[pltpu.VMEM((rows, 2 * cols), BF16), pltpu.VMEM((rows, width), F32)],
        ),
        out_shape=out,
        cost_estimate=cost(4 * rows * width * cols * half, gate, up, own, other, out, *pieces),
        name="dgate",
    )(place, gate, up, own, other, *pieces)


def fresh_kernel(scale, coef, tok_ref, p_ref, left_ref, right_ref, t_ref, fresh_ref, gate_ref):
    k = pl.program_id(0)

    @pl.when(k == 0)
    def _():
        gate_ref[...] = jnp.zeros_like(gate_ref)

    mixed = (
        coef[0] * p_ref[...].astype(F32)
        + coef[1] * right_ref[...].astype(F32)
        + coef[2] * left_ref[...].astype(F32)
    )
    fresh = (mixed - coef[3] * t_ref[...].astype(F32)).astype(BF16)
    fresh_ref[...] = fresh
    gate_ref[...] += jnp.dot(tok_ref[...], fresh, preferred_element_type=F32)

    @pl.when(k == pl.num_programs(0) - 1)
    def _():
        gate_ref[...] = gate_ref[...] * scale


def fresh_of(coef, tok, param, left, right, track, scale):
    depth, width = param.shape
    rows = tok.shape[0]
    step = block_of(depth, 256)
    block = pl.BlockSpec((step, width), lambda k: (k, 0))
    out = [jax.ShapeDtypeStruct((depth, width), BF16), jax.ShapeDtypeStruct((rows, width), F32)]
    return pl.pallas_call(
        functools.partial(fresh_kernel, scale),
        grid=(depth // step,),
        in_specs=[
            pl.BlockSpec(memory_space=pltpu.SMEM),
            pl.BlockSpec((rows, step), lambda k: (0, k)),
            block,
            block,
            block,
            block,
        ],
        out_specs=[block, pl.BlockSpec((rows, width), lambda k: (0, 0))],
        out_shape=out,
        cost_estimate=cost(2 * rows * depth * width, tok, param, left, right, track, *out),
        name="fresh",
    )(coef, tok, param, left, right, track)


def final_kernel(scale, coef, tok_ref, new_ref, old_ref, t_ref, left_ref, right_ref, *rest):
    out_ref = rest[-1]
    tok = tok_ref[...]
    dims = (((0,), (0,)), ((), ()))
    change = lax.dot_general(tok, new_ref[...], dims, preferred_element_type=F32) - lax.dot_general(
        tok, old_ref[...], dims, preferred_element_type=F32
    )
    mixed = (
        coef[0] * t_ref[...].astype(F32)
        + coef[1] * right_ref[...].astype(F32)
        + coef[2] * left_ref[...].astype(F32)
    )
    out_ref[...] = (mixed + change * scale).astype(BF16)


def final_of(coef, tok, new, old, track, left, right, scale, start, so_far):
    depth, width = track.shape
    rows = tok.shape[0]
    part = left.shape[0]
    step = block_of(part, 256)
    base = start // step
    there = pl.BlockSpec((step, width), lambda k: (base + k, 0))
    here = pl.BlockSpec((step, width), lambda k: (k, 0))
    whole = pl.BlockSpec((rows, width), lambda k: (0, 0))
    operands = [coef, tok, new, old, track, left, right]
    specs = [
        pl.BlockSpec(memory_space=pltpu.SMEM),
        pl.BlockSpec((rows, step), lambda k: (0, base + k)),
        whole,
        whole,
        there,
        here,
        here,
    ]
    aliases = {}
    if so_far is not None:
        aliases = {len(operands): 0}
        operands.append(so_far)
        specs.append(pl.BlockSpec(memory_space=pl.ANY))
    out = jax.ShapeDtypeStruct((depth, width), BF16)
    return pl.pallas_call(
        functools.partial(final_kernel, scale),
        grid=(part // step,),
        in_specs=specs,
        out_specs=there,
        out_shape=out,
        input_output_aliases=aliases,
        cost_estimate=cost(4 * rows * part * width, left, right, left, left, new, old),
        name="final",
    )(*operands)


def spread(piece, axis, pairs):
    near = [piece] + [jumped(piece, axis, j) for j in range(1, pairs)]
    return near + [paired(part, axis) for part in near]


def on_device(tokens, targets, params, tracker, up_weight, down_weight, edge_weight, step_size):
    token_rows, target_rows, param, track = tokens[0], targets[0], params[0], tracker[0]
    agents, count = lax.axis_size("agent"), lax.axis_size("tp")
    half, pairs = agents // 2, count // 2
    depth = param.shape[0]
    piece = token_rows.shape[0]
    scale = 1.0 / depth**0.5

    index = lax.axis_index("agent")
    place = jnp.stack([index // 2, index % 2]).astype(jnp.int32)
    e_right = lax.dynamic_slice_in_dim(edge_weight, index, 1)[0]
    e_left = lax.dynamic_slice_in_dim(edge_weight, (index + agents - 1) % agents, 1)[0]
    coef = jnp.stack([1.0 - e_right - e_left, e_right, e_left, step_size[0]])

    def gathered(weight):
        return [weight] + [jumped(weight, "agent", j) for j in range(1, half)]

    ups, downs = gathered(up_weight), gathered(down_weight)
    left_x, right_x = shifted(param, "agent", 1), shifted(param, "agent", -1)
    part = depth // CHUNKS
    around = []
    for c in range(CHUNKS):
        t = track[c * part : (c + 1) * part]
        around.append((shifted(t, "agent", 1), shifted(t, "agent", -1)))

    tok = jnp.concatenate(spread(token_rows, "tp", pairs))
    own_up = jnp.stack(ups)
    other_up = paired(own_up, "agent")
    own_down = jnp.stack(downs)
    other_down = paired(own_down, "agent")
    gate = gate_of(tok, param, scale)
    up = up_of(place, tok, own_up, other_up)

    def errors(gate):
        near, *far = share_of(place, gate, up, own_down, other_down, pairs)
        order = list(range(1, pairs)) + [0]
        sent = {j: paired(far[j], "tp") for j in order}

        def joined(j):
            mine = near[j * piece : (j + 1) * piece].astype(F32)
            return mine + sent[j].astype(F32)

        summed = []
        for j in range(1, pairs):
            value = lax.optimization_barrier(joined(j).astype(BF16))
            summed.append(jumped(value, "tp", -j))
        total = joined(0)
        for value in summed:
            total = total + value.astype(F32)
        err = (2.0 * (total - target_rows.astype(F32))).astype(BF16)
        return spread(err, "tp", pairs)

    def dgate(gate, pieces):
        return dgate_of(place, gate, up, own_down, other_down, pieces)

    old_pieces = errors(gate)
    later, old_pieces[0] = lax.optimization_barrier((coef, old_pieces[0]))
    fresh, new_gate = fresh_of(later, tok, param, left_x, right_x, track, scale)
    new_pieces = errors(new_gate)
    old = dgate(gate, old_pieces)
    new = dgate(new_gate, new_pieces)
    out = None
    for c, (left_y, right_y) in enumerate(around):
        out = final_of(coef, tok, new, old, track, left_y, right_y, scale, c * part, out)
    return (fresh[None], out[None])


def solution(mesh):
    return jax.shard_map(
        on_device,
        mesh=mesh,
        in_specs=(
            P("agent", "tp", None),
            P("agent", "tp", None),
            P("agent", None, "tp"),
            P("agent", None, "tp"),
            P("agent", "tp"),
            P("tp", "agent"),
            P(),
            P(),
        ),
        out_specs=(P("agent", None, "tp"), P("agent", None, "tp")),
        check_vma=False,
    )
```

```python
import functools

import jax
import jax.numpy as jnp
from jax import lax
from jax.experimental import pallas as pl
from jax.experimental.pallas import tpu as pltpu
from jax.sharding import PartitionSpec as P


F32 = jnp.float32
BF16 = jnp.bfloat16
PARTS = (4, 4, 4, 2, 2)
VMEM_LIMIT = 67043328


def shifted(value, axis, shift):
    count = lax.axis_size(axis)
    return lax.ppermute(value, axis, [(source, (source + shift) % count) for source in range(count)])


def paired(value, axis):
    return lax.ppermute(value, axis, [(source, source ^ 1) for source in range(lax.axis_size(axis))])


def jumped(value, axis, shift):
    return shifted(value, axis, 2 * shift)


def cost(flops, *arrays):
    return pl.CostEstimate(
        flops=flops, bytes_accessed=sum(a.size * a.dtype.itemsize for a in arrays), transcendentals=0
    )


def block_of(size, most):
    return most if size % most == 0 else size


def column_blocks(width):
    if width % 512 == 0:
        return [0, width // 2, 3 * width // 4, width]
    return [0, width // 2, width] if width % 256 == 0 else [0, width]


def like(shape, dtype):
    return jax.ShapeDtypeStruct(shape, dtype)


def dot(a, b, contract=(1, 0)):
    return lax.dot_general(a, b, (((contract[0],), (contract[1],)), ((), ())), preferred_element_type=F32)


SMEM = pl.BlockSpec(memory_space=pltpu.SMEM)
call = functools.partial(pl.pallas_call, compiler_params=pltpu.CompilerParams(vmem_limit_bytes=VMEM_LIMIT))


def columns(place, i, size):
    return pl.ds(pl.multiple_of(place[i] * size, size), size)


def pack_kernel(*refs):
    *pieces, out_ref, turned_ref = refs
    rows = pieces[0].shape[0]
    for k, ref in enumerate(pieces):
        out_ref[k * rows : (k + 1) * rows, :] = ref[...]
    turned_ref[...] = out_ref[...].T


def pack(pieces):
    rows, width = pieces[0].shape
    rows *= len(pieces)
    dtype = pieces[0].dtype
    return call(pack_kernel, out_shape=[like((rows, width), dtype), like((width, rows), dtype)], name="pack")(
        *pieces
    )


def gate_kernel(scale, tok_ref, w_ref, out_ref):
    out_ref[...] = dot(tok_ref[...], w_ref[...]) * scale


def gate_of(tok, weights, scale):
    rows, depth = tok.shape
    width = weights.shape[1]
    cols = block_of(width, 512)
    out = like((rows, width), F32)
    return call(
        functools.partial(gate_kernel, scale),
        grid=(width // cols,),
        in_specs=[
            pl.BlockSpec((rows, depth), lambda i: (0, 0)),
            pl.BlockSpec((depth, cols), lambda i: (0, i)),
        ],
        out_specs=pl.BlockSpec((rows, cols), lambda i: (0, i)),
        out_shape=out,
        cost_estimate=cost(2 * rows * depth * width, tok, weights, out),
        name="gate",
    )(tok, weights)


def up_kernel(place, tok_ref, *refs):
    total = None
    for i, ref in enumerate(refs[:-1]):
        term = dot(tok_ref[:, columns(place, i, ref.shape[0])], ref[...])
        total = term if total is None else total + term
    refs[-1][...] = total


def up_of(place, tok, pieces):
    depth, width = pieces[0].shape
    rows = tok.shape[0]
    cols = block_of(width, 256)
    out = like((rows, width), F32)
    return call(
        up_kernel,
        grid=(width // cols,),
        in_specs=[SMEM, pl.BlockSpec(tok.shape, lambda n: (0, 0))]
        + [pl.BlockSpec((depth, cols), lambda n: (0, n))] * len(pieces),
        out_specs=pl.BlockSpec((rows, cols), lambda n: (0, n)),
        out_shape=out,
        cost_estimate=cost(2 * rows * depth * width * len(pieces), tok, out, *pieces),
        name="up",
    )(place, tok, *pieces)


def add_share(place, gate, up_ref, weights, carry, outs, total):
    hidden = (jax.nn.sigmoid(gate) * gate * up_ref[...]).astype(BF16)
    n, last = pl.program_id(0), pl.num_programs(0) - 1
    for i, ref in enumerate(weights):
        term = dot(hidden, ref[...])

        @pl.when(n == 0)
        def _():
            total[i] = term if carry is None else carry[i] + term

        @pl.when(n > 0)
        def _():
            total[i] += term

    if not outs:
        return

    @pl.when(n == last)
    def _():
        cols = weights[0].shape[1]
        for i in range(len(weights)):
            start = 0
            for ref in outs:
                stop = start + ref.shape[0]
                ref[:, columns(place, i, cols)] = total[i, start:stop, :].astype(BF16)
                start = stop


def share_kernel(count, place, gate_ref, up_ref, *refs):
    add_share(place, gate_ref[...], up_ref, refs[:count], None, refs[count:-1], refs[-1])


def share_outs(rows, depth, pairs):
    near, piece = rows // 2, rows // 2 // pairs
    outs = [like((near, depth), BF16)] + [like((piece, depth), BF16)] * pairs
    return outs, [pl.BlockSpec(o.shape, lambda n: (0, 0)) for o in outs]


def share_of(place, gate, up, downs, pairs):
    rows, width = gate.shape
    cols = downs[0].shape[1]
    depth = cols * len(downs)
    block = block_of(width, 256)
    spec = pl.BlockSpec((rows, block), lambda n: (0, n))
    outs, out_specs = share_outs(rows, depth, pairs)
    return call(
        functools.partial(share_kernel, len(downs)),
        grid=(width // block,),
        in_specs=[SMEM, spec, spec] + [pl.BlockSpec((block, cols), lambda n: (n, 0))] * len(downs),
        out_specs=out_specs,
        out_shape=outs,
        scratch_shapes=[pltpu.VMEM((len(downs), rows, cols), F32)],
        cost_estimate=cost(2 * rows * width * depth, gate, up, *downs, *outs),
        name="share",
    )(place, gate, up, *downs)


def fresh_kernel(count, scale, first, last, place, coef, tok_ref, p_ref, left_ref, right_ref, t_ref, up_ref, *refs):
    weights, refs = refs[:count], refs[count:]
    carry = None
    if not first:
        carry, refs = refs[0], refs[3:]
    fresh_ref, gate_ref, *refs = refs
    mixed = (
        coef[0] * p_ref[...].astype(F32)
        + coef[1] * right_ref[...].astype(F32)
        + coef[2] * left_ref[...].astype(F32)
    )
    fresh = (mixed - coef[3] * t_ref[...].astype(F32)).astype(BF16)
    fresh_ref[...] = fresh
    gate = dot(tok_ref[...], fresh) * scale
    gate_ref[...] = gate
    outs, total = (refs[:-1], refs[-1]) if last else ([], refs[0])
    add_share(place, gate, up_ref, weights, carry, outs, total)


def fresh_of(place, coef, tok, param, left, right, track, up, downs, pairs, scale, start, so_far):
    depth, width = param.shape
    rows, part = tok.shape[0], left.shape[1]
    cols = downs[0].shape[1]
    block = block_of(part, 256)
    base = start // block
    first, last = so_far is None, start + part == width
    there = pl.BlockSpec((depth, block), lambda n: (0, base + n))
    here = pl.BlockSpec((depth, block), lambda n: (0, n))
    hidden = pl.BlockSpec((rows, block), lambda n: (0, base + n))
    operands = [place, coef, tok, param, left, right, track, up, *downs]
    specs = [SMEM, SMEM, pl.BlockSpec(tok.shape, lambda n: (0, 0)), there, here, here, there, hidden]
    specs += [pl.BlockSpec((block, cols), lambda n: (base + n, 0))] * len(downs)
    total = (len(downs), rows, cols)
    whole = pl.BlockSpec(total, lambda n: (0, 0, 0))
    aliases = {}
    if not first:
        aliases = {len(operands) + 1: 0, len(operands) + 2: 1}
        operands += [so_far[2], so_far[0], so_far[1]]
        specs += [whole, pl.BlockSpec(memory_space=pl.ANY), pl.BlockSpec(memory_space=pl.ANY)]
    outs, out_specs = [like((depth, width), BF16), like((rows, width), F32)], [there, hidden]
    scratch = []
    if last:
        more, more_specs = share_outs(rows, cols * len(downs), pairs)
        outs, out_specs = outs + more, out_specs + more_specs
        scratch = [pltpu.VMEM(total, F32)]
    else:
        outs, out_specs = outs + [like(total, F32)], out_specs + [whole]
    return call(
        functools.partial(fresh_kernel, len(downs), scale, first, last),
        grid=(part // block,),
        in_specs=specs,
        out_specs=out_specs,
        out_shape=outs,
        scratch_shapes=scratch,
        input_output_aliases=aliases,
        cost_estimate=cost(4 * rows * depth * part, left, left, right, right, left, up, *downs),
        name="fresh",
    )(*operands)


def join_kernel(mine_ref, other_ref, out_ref):
    out_ref[...] = (mine_ref[...].astype(F32) + other_ref[...].astype(F32)).astype(BF16)


def join(near, other, j):
    out = like(other.shape, BF16)
    whole = pl.BlockSpec(other.shape, lambda i: (0, 0))
    return call(
        join_kernel,
        grid=(1,),
        in_specs=[pl.BlockSpec(other.shape, lambda i: (j, 0)), whole],
        out_specs=whole,
        out_shape=out,
        cost_estimate=cost(out.size, other, other, out),
        name="join",
    )(near, other)


def dgate_block(count, place, gate_ref, up_ref, refs, err):
    weights, pieces = refs[:count], refs[count:]

    @pl.when(pl.program_id(0) == 0)
    def _():
        rows = pieces[0].shape[0]
        for k, ref in enumerate(pieces):
            err[k * rows : (k + 1) * rows, :] = ref[...]

    back = None
    for i, ref in enumerate(weights):
        term = dot(err[:, columns(place, i, ref.shape[1])], ref[...], (1, 1))
        back = term if back is None else back + term
    gate = gate_ref[...]
    sig = jax.nn.sigmoid(gate)
    return (back * up_ref[...] * sig * (1.0 + gate * (1.0 - sig))).astype(BF16)


def dgate_kernel(count, place, gate_ref, up_ref, *refs):
    refs[-2][...] = dgate_block(count, place, gate_ref, up_ref, refs[:-2], refs[-1])


def tail_kernel(count, scale, place, turned_ref, base_ref, gate_ref, up_ref, *refs):
    *refs, dgate_ref, out_ref, err = refs
    value = dgate_block(count, place, gate_ref, up_ref, refs, err)
    dgate_ref[...] = value
    out_ref[...] = (base_ref[...] + dot(turned_ref[...], value) * scale).astype(BF16)


def dgate_of(place, gate, up, downs, pieces, more=None):
    width, cols = downs[0].shape
    rows = gate.shape[0]
    block = block_of(width, 256)
    hidden = pl.BlockSpec((rows, block), lambda n: (0, n))
    whole = pl.BlockSpec(pieces[0].shape, lambda n: (0, 0))
    depth = cols * len(downs)
    operands, specs = [place], [SMEM]
    outs, out_specs = [like((rows, width), BF16)], [hidden]
    kernel, flops = functools.partial(dgate_kernel, len(downs)), 2 * rows * width * depth
    if more is not None:
        turned, base, out, scale = more
        tall = pl.BlockSpec((base.shape[0], block), lambda n: (0, n))
        operands += [turned, base]
        specs += [pl.BlockSpec((base.shape[0], rows), lambda n: (0, 0)), tall]
        outs, out_specs = outs + [out], out_specs + [tall]
        kernel, flops = functools.partial(tail_kernel, len(downs), scale), 2 * flops
    return call(
        kernel,
        grid=(width // block,),
        in_specs=specs
        + [hidden, hidden]
        + [pl.BlockSpec((block, cols), lambda n: (n, 0))] * len(downs)
        + [whole] * len(pieces),
        out_specs=out_specs,
        out_shape=outs,
        scratch_shapes=[pltpu.VMEM((rows, depth), BF16)],
        cost_estimate=cost(flops, gate, up, *outs, *downs, *pieces),
        name="dgate",
    )(*operands, gate, up, *downs, *pieces)


def base_kernel(scale, coef, turned_ref, old_ref, t_ref, left_ref, right_ref, *rest):
    mixed = (
        coef[0] * t_ref[...].astype(F32)
        + coef[1] * right_ref[...].astype(F32)
        + coef[2] * left_ref[...].astype(F32)
    )
    rest[-1][...] = mixed - dot(turned_ref[...], old_ref[...]) * scale


def last_kernel(scale, coef, turned_ref, new_ref, old_ref, t_ref, left_ref, right_ref, *rest):
    turned = turned_ref[...]
    change = dot(turned, new_ref[...]) - dot(turned, old_ref[...])
    mixed = (
        coef[0] * t_ref[...].astype(F32)
        + coef[1] * right_ref[...].astype(F32)
        + coef[2] * left_ref[...].astype(F32)
    )
    rest[-1][...] = (mixed + change * scale).astype(BF16)


def part_call(kernel, coef, turned, grads, track, left, right, start, out, so_far, name):
    width = track.shape[1]
    rows, part = turned.shape[1], left.shape[0]
    step = block_of(part, 256)
    base = start // step
    there = pl.BlockSpec((step, width), lambda k: (base + k, 0))
    here = pl.BlockSpec((step, width), lambda k: (k, 0))
    whole = pl.BlockSpec((rows, width), lambda k: (0, 0))
    operands = [coef, turned, *grads, track, left, right]
    specs = [SMEM, pl.BlockSpec((step, rows), lambda k: (base + k, 0))]
    specs += [whole] * len(grads) + [there, here, here]
    aliases = {}
    if so_far is not None:
        aliases = {len(operands): 0}
        operands.append(so_far)
        specs.append(pl.BlockSpec(memory_space=pl.ANY))
    return call(
        kernel,
        grid=(part // step,),
        in_specs=specs,
        out_specs=there,
        out_shape=out,
        input_output_aliases=aliases,
        cost_estimate=cost(2 * len(grads) * rows * part * width, left, right, left, left, *grads),
        name=name,
    )(*operands)


def spread(piece, axis, pairs):
    near = [piece] + [jumped(piece, axis, j) for j in range(1, pairs)]
    return near + [paired(part, axis) for part in near]


def on_device(tokens, targets, params, tracker, up_weight, down_weight, edge_weight, step_size):
    token_rows, target_rows, param, track = tokens[0], targets[0], params[0], tracker[0]
    agents, count = lax.axis_size("agent"), lax.axis_size("tp")
    half, pairs = agents // 2, count // 2
    depth = param.shape[0]
    piece = token_rows.shape[0]
    scale = 1.0 / depth**0.5

    index = lax.axis_index("agent")
    even, parity = index // 2, index % 2
    chips = [lax.rem(even - j + half, half) for j in range(half)]
    place = jnp.stack([2 * c + parity for c in chips] + [2 * c + 1 - parity for c in chips]).astype(jnp.int32)
    e_right = lax.dynamic_slice_in_dim(edge_weight, index, 1)[0]
    e_left = lax.dynamic_slice_in_dim(edge_weight, (index + agents - 1) % agents, 1)[0]
    coef = jnp.stack([1.0 - e_right - e_left, e_right, e_left, step_size[0]])

    def gathered(weight):
        own = [weight] + [jumped(weight, "agent", j) for j in range(1, half)]
        return own + [paired(w, "agent") for w in own]

    ups, downs = gathered(up_weight), gathered(down_weight)
    edges = column_blocks(param.shape[1])
    blocks = len(edges) - 1
    sides = []
    for start, end in zip(edges, edges[1:]):
        p = param[:, start:end]
        sides.append((shifted(p, "agent", 1), shifted(p, "agent", -1)))
    ends = [depth * sum(PARTS[: c + 1]) // sum(PARTS) for c in range(len(PARTS))]
    starts = [0] + ends[:-1]
    around = []
    for start, end in zip(starts, ends):
        t = track[start:end]
        around.append((shifted(t, "agent", 1), shifted(t, "agent", -1)))

    tok, turned = pack(spread(token_rows, "tp", pairs))
    gate = gate_of(tok, param, scale)
    up = up_of(place, tok, ups)

    def errors(shares):
        near, *far = shares
        order = list(range(1, pairs)) + [0]
        sent = {j: paired(far[j], "tp") for j in order}
        summed = []
        for j in range(1, pairs):
            value = join(near, sent[j], j)
            summed.append(jumped(value, "tp", -j))
        total = near[:piece].astype(F32) + sent[0].astype(F32)
        for value in summed:
            total = total + value.astype(F32)
        err = (2.0 * (total - target_rows.astype(F32))).astype(BF16)
        return spread(err, "tp", pairs)

    shares = share_of(place, gate, up, downs, pairs)
    made = None
    for h in range(blocks - 1):
        made = fresh_of(
            place, coef, tok, param, *sides[h], track, up, downs, pairs, scale, edges[h], made
        )
    old_pieces = errors(shares)
    later, old_pieces[0] = lax.optimization_barrier((coef, old_pieces[0]))
    fresh, new_gate, *shares = fresh_of(
        place, later, tok, param, *sides[-1], track, up, downs, pairs, scale, edges[-2], made
    )
    new_pieces = errors(shares)
    (old,) = dgate_of(place, gate, up, downs, old_pieces)
    base = None
    early_like, all_like = like((starts[-1], track.shape[1]), F32), like(track.shape, BF16)
    for c in range(len(PARTS) - 1):
        kernel = functools.partial(base_kernel, scale)
        base = part_call(kernel, coef, turned, [old], track, *around[c], starts[c], early_like, base, "base")
    new, out = dgate_of(place, new_gate, up, downs, new_pieces, (turned, base, all_like, scale))
    kernel = functools.partial(last_kernel, scale)
    out = part_call(
        kernel, coef, turned, [new, old], track, *around[-1], starts[-1], all_like, out, "last"
    )
    return (fresh[None], out[None])


def solution(mesh):
    return jax.shard_map(
        on_device,
        mesh=mesh,
        in_specs=(
            P("agent", "tp", None),
            P("agent", "tp", None),
            P("agent", None, "tp"),
            P("agent", None, "tp"),
            P("agent", "tp"),
            P("tp", "agent"),
            P(),
            P(),
        ),
        out_specs=(P("agent", None, "tp"), P("agent", None, "tp")),
        check_vma=False,
    )
```

```python
import functools
import math

import jax
import jax.numpy as jnp
from jax import lax
from jax.experimental import pallas as pl
from jax.experimental.pallas import tpu as pltpu
from jax.sharding import PartitionSpec as P


F32 = jnp.float32
BF16 = jnp.bfloat16
PARTS = (4, 6, 4, 2)
VMEM_LIMIT = 67043328


def shifted(value, axis, shift):
    count = lax.axis_size(axis)
    return lax.ppermute(value, axis, [(source, (source + shift) % count) for source in range(count)])


def paired(value, axis):
    return lax.ppermute(value, axis, [(source, source ^ 1) for source in range(lax.axis_size(axis))])


def jumped(value, axis, shift):
    return shifted(value, axis, 2 * shift)


def cost(flops, *arrays):
    return pl.CostEstimate(
        flops=flops, bytes_accessed=sum(a.size * a.dtype.itemsize for a in arrays), transcendentals=0
    )


def block_of(size, most):
    return most if size % most == 0 else size


def column_blocks(width):
    if width % 512 == 0:
        return [0, width // 2, 3 * width // 4, width]
    return [0, width // 2, width] if width % 256 == 0 else [0, width]


def like(shape, dtype):
    return jax.ShapeDtypeStruct(shape, dtype)


def dot(a, b, contract=(1, 0)):
    return lax.dot_general(a, b, (((contract[0],), (contract[1],)), ((), ())), preferred_element_type=F32)


SMEM = pl.BlockSpec(memory_space=pltpu.SMEM)
ANY = pl.BlockSpec(memory_space=pl.ANY)


def call(kernel, **options):
    return pl.pallas_call(kernel, compiler_params=pltpu.CompilerParams(vmem_limit_bytes=VMEM_LIMIT), **options)


def columns(place, i, size):
    return pl.ds(pl.multiple_of(place[i] * size, size), size)


def pack_kernel(*refs):
    *pieces, out_ref, turned_ref = refs
    rows = pieces[0].shape[0]
    for k, ref in enumerate(pieces):
        out_ref[k * rows : (k + 1) * rows, :] = ref[...]
    turned_ref[...] = out_ref[...].T


def pack(pieces):
    rows, width = pieces[0].shape
    rows *= len(pieces)
    dtype = pieces[0].dtype
    return call(pack_kernel, out_shape=[like((rows, width), dtype), like((width, rows), dtype)], name="pack")(
        *pieces
    )


def gate_kernel(scale, tok_ref, w_ref, out_ref):
    out_ref[...] = dot(tok_ref[...], w_ref[...]) * scale


def gate_of(tok, weights, scale):
    rows, depth = tok.shape
    width = weights.shape[1]
    cols = block_of(width, 512)
    out = like((rows, width), F32)
    return call(
        functools.partial(gate_kernel, scale),
        grid=(width // cols,),
        in_specs=[
            pl.BlockSpec((rows, depth), lambda i: (0, 0)),
            pl.BlockSpec((depth, cols), lambda i: (0, i)),
        ],
        out_specs=pl.BlockSpec((rows, cols), lambda i: (0, i)),
        out_shape=out,
        cost_estimate=cost(2 * rows * depth * width, tok, weights, out),
        name="gate",
    )(tok, weights)


def up_kernel(place, tok_ref, *refs):
    total = None
    for i, ref in enumerate(refs[:-1]):
        term = dot(tok_ref[:, columns(place, i, ref.shape[0])], ref[...])
        total = term if total is None else total + term
    refs[-1][...] = total


def up_of(place, tok, pieces):
    depth, width = pieces[0].shape
    rows = tok.shape[0]
    cols = block_of(width, 256)
    out = like((rows, width), F32)
    return call(
        up_kernel,
        grid=(width // cols,),
        in_specs=[SMEM, pl.BlockSpec(tok.shape, lambda n: (0, 0))]
        + [pl.BlockSpec((depth, cols), lambda n: (0, n))] * len(pieces),
        out_specs=pl.BlockSpec((rows, cols), lambda n: (0, n)),
        out_shape=out,
        cost_estimate=cost(2 * rows * depth * width * len(pieces), tok, out, *pieces),
        name="up",
    )(place, tok, *pieces)


def add_share(place, gate, up_ref, weights, carry, bring, outs, total):
    hidden = (jax.nn.sigmoid(gate) * gate * up_ref[...]).astype(BF16)
    n, last = pl.program_id(0), pl.num_programs(0) - 1
    if bring is not None:

        @pl.when(n == 0)
        def _():
            bring.wait()

    for i, ref in enumerate(weights):
        term = dot(hidden, ref[...])
        if bring is not None:
            total[i] += term
            continue

        @pl.when(n == 0)
        def _():
            total[i] = term if carry is None else carry[i] + term

        @pl.when(n > 0)
        def _():
            total[i] += term

    if not outs:
        return

    @pl.when(n == last)
    def _():
        cols = weights[0].shape[1]
        for i in range(len(weights)):
            start = 0
            for ref in outs:
                stop = start + ref.shape[0]
                ref[:, columns(place, i, cols)] = total[i, start:stop, :].astype(BF16)
                start = stop


def share_kernel(count, place, gate_ref, up_ref, *refs):
    add_share(place, gate_ref[...], up_ref, refs[:count], None, None, refs[count:-1], refs[-1])


def share_outs(rows, depth, pairs):
    near, piece = rows // 2, rows // 2 // pairs
    outs = [like((near, depth), BF16)] + [like((piece, depth), BF16)] * pairs
    return outs, [pl.BlockSpec(o.shape, lambda n: (0, 0)) for o in outs]


def share_of(place, gate, up, downs, pairs):
    rows, width = gate.shape
    cols = downs[0].shape[1]
    depth = cols * len(downs)
    block = block_of(width, 256)
    spec = pl.BlockSpec((rows, block), lambda n: (0, n))
    outs, out_specs = share_outs(rows, depth, pairs)
    return call(
        functools.partial(share_kernel, len(downs)),
        grid=(width // block,),
        in_specs=[SMEM, spec, spec] + [pl.BlockSpec((block, cols), lambda n: (n, 0))] * len(downs),
        out_specs=out_specs,
        out_shape=outs,
        scratch_shapes=[pltpu.VMEM((len(downs), rows, cols), F32)],
        cost_estimate=cost(2 * rows * width * depth, gate, up, *downs, *outs),
        name="share",
    )(place, gate, up, *downs)


def fresh_kernel(count, scale, first, last, place, coef, tok_ref, p_ref, left_ref, right_ref, t_ref, up_ref, *refs):
    weights, refs = refs[:count], refs[count:]
    carry = bring = None
    if not first:
        carry, refs = refs[0], refs[3:]
    if carry is not None and last:
        bring, refs = pltpu.make_async_copy(carry, refs[-2], refs[-1]), refs[:-1]

        @pl.when(pl.program_id(0) == 0)
        def _():
            bring.start()

    fresh_ref, gate_ref, *refs = refs
    mixed = (
        coef[0] * p_ref[...].astype(F32)
        + coef[1] * right_ref[...].astype(F32)
        + coef[2] * left_ref[...].astype(F32)
    )
    fresh = (mixed - coef[3] * t_ref[...].astype(F32)).astype(BF16)
    fresh_ref[...] = fresh
    gate = dot(tok_ref[...], fresh) * scale
    gate_ref[...] = gate
    add_share(place, gate, up_ref, weights, carry, bring, refs[:-1], refs[-1])


def fresh_of(place, coef, tok, param, left, right, track, up, downs, pairs, scale, start, so_far):
    depth, width = param.shape
    rows, part = tok.shape[0], left.shape[1]
    cols = downs[0].shape[1]
    block = math.gcd(256, start, part)
    base = start // block
    first, last = so_far is None, start + part == width
    there = pl.BlockSpec((depth, block), lambda n: (0, base + n))
    here = pl.BlockSpec((depth, block), lambda n: (0, n))
    hidden = pl.BlockSpec((rows, block), lambda n: (0, base + n))
    operands = [place, coef, tok, param, left, right, track, up, *downs]
    specs = [SMEM, SMEM, pl.BlockSpec(tok.shape, lambda n: (0, 0)), there, here, here, there, hidden]
    specs += [pl.BlockSpec((block, cols), lambda n: (base + n, 0))] * len(downs)
    total = (len(downs), rows, cols)
    whole = pl.BlockSpec(total, lambda n: (0, 0, 0))
    aliases = {}
    if not first:
        aliases = {len(operands) + 1: 0, len(operands) + 2: 1}
        operands += [so_far[2], so_far[0], so_far[1]]
        specs += [ANY if last else whole, ANY, ANY]
    outs, out_specs = [like((depth, width), BF16), like((rows, width), F32)], [there, hidden]
    scratch = []
    if last:
        more, more_specs = share_outs(rows, cols * len(downs), pairs)
        outs, out_specs = outs + more, out_specs + more_specs
        scratch = [pltpu.VMEM(total, F32)] + ([] if first else [pltpu.SemaphoreType.DMA(())])
    else:
        outs, out_specs = outs + [like(total, F32)], out_specs + [whole]
    return call(
        functools.partial(fresh_kernel, len(downs), scale, first, last),
        grid=(part // block,),
        in_specs=specs,
        out_specs=out_specs,
        out_shape=outs,
        scratch_shapes=scratch,
        input_output_aliases=aliases,
        cost_estimate=cost(4 * rows * depth * part, left, left, right, right, left, up, *downs),
        name="fresh",
    )(*operands)


def join_kernel(mine_ref, other_ref, out_ref):
    out_ref[...] = (mine_ref[...].astype(F32) + other_ref[...].astype(F32)).astype(BF16)


def join(near, other, j):
    out = like(other.shape, BF16)
    whole = pl.BlockSpec(other.shape, lambda i: (0, 0))
    return call(
        join_kernel,
        grid=(1,),
        in_specs=[pl.BlockSpec(other.shape, lambda i: (j, 0)), whole],
        out_specs=whole,
        out_shape=out,
        cost_estimate=cost(out.size, other, other, out),
        name="join",
    )(near, other)


def dgate_block(count, place, gate_ref, up_ref, refs, err):
    weights, pieces = refs[:count], refs[count:]

    @pl.when(pl.program_id(0) == 0)
    def _():
        rows = pieces[0].shape[0]
        for k, ref in enumerate(pieces):
            err[k * rows : (k + 1) * rows, :] = ref[...]

    back = None
    for i, ref in enumerate(weights):
        term = dot(err[:, columns(place, i, ref.shape[1])], ref[...], (1, 1))
        back = term if back is None else back + term
    gate = gate_ref[...]
    sig = jax.nn.sigmoid(gate)
    return (back * up_ref[...] * sig * (1.0 + gate * (1.0 - sig))).astype(BF16)


def dgate_kernel(count, place, gate_ref, up_ref, *refs):
    refs[-2][...] = dgate_block(count, place, gate_ref, up_ref, refs[:-2], refs[-1])


def tail_kernel(count, scale, place, turned_hbm, base_ref, gate_ref, up_ref, *refs):
    *refs, out_ref, late_ref, err, turned, turned_sem = refs
    bring_turned = pltpu.make_async_copy(turned_hbm, turned, turned_sem)
    first = pl.program_id(0) == 0

    @pl.when(first)
    def _():
        bring_turned.start()

    value = dgate_block(count, place, gate_ref, up_ref, refs, err)

    @pl.when(first)
    def _():
        bring_turned.wait()

    rows = out_ref.shape[0]
    total = base_ref[...] + dot(turned[...], value) * scale
    out_ref[...] = total[:rows].astype(BF16)
    late_ref[...] = total[rows:]


def dgate_of(place, gate, up, downs, pieces, more=None):
    width, cols = downs[0].shape
    rows = gate.shape[0]
    block = block_of(width, 256)
    hidden = pl.BlockSpec((rows, block), lambda n: (0, n))
    whole = pl.BlockSpec(pieces[0].shape, lambda n: (0, 0))
    depth = cols * len(downs)
    operands, specs, scratch = [place], [SMEM], [pltpu.VMEM((rows, depth), BF16)]
    outs, out_specs = [like((rows, width), BF16)], [hidden]
    kernel, flops = functools.partial(dgate_kernel, len(downs)), 2 * rows * width * depth
    if more is not None:
        turned, base, out, done, scale = more
        tall = base.shape[0]
        operands += [turned, base]
        specs += [ANY, pl.BlockSpec((tall, block), lambda n: (0, n))]
        scratch += [pltpu.VMEM(turned.shape, turned.dtype), pltpu.SemaphoreType.DMA(())]
        outs = [out, like((tall - done, width), F32)]
        out_specs = [pl.BlockSpec((size, block), lambda n: (0, n)) for size in (done, tall - done)]
        kernel, flops = functools.partial(tail_kernel, len(downs), scale), 2 * flops
    return call(
        kernel,
        grid=(width // block,),
        in_specs=specs
        + [hidden, hidden]
        + [pl.BlockSpec((block, cols), lambda n: (n, 0))] * len(downs)
        + [whole] * len(pieces),
        out_specs=out_specs,
        out_shape=outs,
        scratch_shapes=scratch,
        cost_estimate=cost(flops, gate, up, *outs, *downs, *pieces),
        name="dgate",
    )(*operands, gate, up, *downs, *pieces)


def base_kernel(scale, coef, turned_ref, old_ref, t_ref, *rest):
    mixed = coef[0] * t_ref[...].astype(F32)
    if len(rest) > 2:
        mixed = mixed + coef[1] * rest[1][...].astype(F32) + coef[2] * rest[0][...].astype(F32)
    rest[-1][...] = mixed - dot(turned_ref[...], old_ref[...]) * scale


def base_of(coef, turned, old, track, sides, start, part, so_far, scale):
    depth, width = track.shape
    rows = turned.shape[1]
    step = math.gcd(256, start, part)
    base = start // step
    there = pl.BlockSpec((step, width), lambda k: (base + k, 0))
    here = pl.BlockSpec((step, width), lambda k: (k, 0))
    operands = [coef, turned, old, track, *sides]
    specs = [SMEM, pl.BlockSpec((step, rows), lambda k: (base + k, 0))]
    specs += [pl.BlockSpec((rows, width), lambda k: (0, 0)), there] + [here] * len(sides)
    aliases = {}
    if so_far is not None:
        aliases = {len(operands): 0}
        operands.append(so_far)
        specs.append(ANY)
    return call(
        functools.partial(base_kernel, scale),
        grid=(part // step,),
        in_specs=specs,
        out_specs=there,
        out_shape=like((depth, width), F32),
        input_output_aliases=aliases,
        cost_estimate=cost(2 * rows * part * width, like((part, width), F32), old, *sides),
        name="base",
    )(*operands)


def last_kernel(coef, late_ref, left_ref, right_ref, so_far, out_ref):
    mixed = coef[1] * right_ref[...].astype(F32) + coef[2] * left_ref[...].astype(F32)
    out_ref[...] = (late_ref[...] + mixed).astype(BF16)


def last_of(coef, late, left, right, out):
    part, width = late.shape
    start = out.shape[0] - part
    step = math.gcd(128, start, part)
    base = start // step
    here = pl.BlockSpec((step, width), lambda k: (k, 0))
    return call(
        last_kernel,
        grid=(part // step,),
        in_specs=[SMEM, here, here, here, ANY],
        out_specs=pl.BlockSpec((step, width), lambda k: (base + k, 0)),
        out_shape=like(out.shape, BF16),
        input_output_aliases={4: 0},
        cost_estimate=cost(late.size, late, left, right, left),
        name="last",
    )(coef, late, left, right, out)


def spread(piece, axis, pairs):
    near = [piece] + [jumped(piece, axis, j) for j in range(1, pairs)]
    return near + [paired(part, axis) for part in near]


def on_device(tokens, targets, params, tracker, up_weight, down_weight, edge_weight, step_size):
    token_rows, target_rows, param, track = tokens[0], targets[0], params[0], tracker[0]
    agents, count = lax.axis_size("agent"), lax.axis_size("tp")
    half, pairs = agents // 2, count // 2
    depth = param.shape[0]
    piece = token_rows.shape[0]
    scale = 1.0 / depth**0.5

    index = lax.axis_index("agent")
    even, parity = index // 2, index % 2
    chips = [lax.rem(even - j + half, half) for j in range(half)]
    place = jnp.stack([2 * c + parity for c in chips] + [2 * c + 1 - parity for c in chips]).astype(jnp.int32)
    e_right = lax.dynamic_slice_in_dim(edge_weight, index, 1)[0]
    e_left = lax.dynamic_slice_in_dim(edge_weight, (index + agents - 1) % agents, 1)[0]
    coef = jnp.stack([1.0 - e_right - e_left, e_right, e_left, step_size[0]])

    def gathered(weight):
        own = [weight] + [jumped(weight, "agent", j) for j in range(1, half)]
        return own + [paired(w, "agent") for w in own]

    ups, downs = gathered(up_weight), gathered(down_weight)
    edges = column_blocks(param.shape[1])
    blocks = len(edges) - 1
    sides = []
    for start, end in zip(edges, edges[1:]):
        p = param[:, start:end]
        sides.append((shifted(p, "agent", 1), shifted(p, "agent", -1)))
    ends = [depth * sum(PARTS[: c + 1]) // sum(PARTS) for c in range(len(PARTS))]
    starts = [0] + ends[:-1]
    around = []
    for start, end in zip(starts, ends):
        t = track[start:end]
        around.append((shifted(t, "agent", 1), shifted(t, "agent", -1)))

    tok, turned = pack(spread(token_rows, "tp", pairs))
    gate = gate_of(tok, param, scale)
    up = up_of(place, tok, ups)

    def errors(shares):
        near, *far = shares
        order = list(range(1, pairs)) + [0]
        sent = {j: paired(far[j], "tp") for j in order}
        summed = []
        for j in order[:-1]:
            value = join(near, sent[j], j)
            summed.append(jumped(value, "tp", -j))
        total = near[:piece].astype(F32) + sent[0].astype(F32)
        for value in summed:
            total = total + value.astype(F32)
        err = (2.0 * (total - target_rows.astype(F32))).astype(BF16)
        return spread(err, "tp", pairs)

    shares = share_of(place, gate, up, downs, pairs)
    made = None
    for h in range(blocks - 1):
        made = fresh_of(
            place, coef, tok, param, *sides[h], track, up, downs, pairs, scale, edges[h], made
        )
    old_pieces = errors(shares)
    later, old_pieces[0] = lax.optimization_barrier((coef, old_pieces[0]))
    fresh, new_gate, *shares = fresh_of(
        place, later, tok, param, *sides[-1], track, up, downs, pairs, scale, edges[-2], made
    )
    new_pieces = errors(shares)
    (old,) = dgate_of(place, gate, up, downs, old_pieces)
    base = None
    final = len(PARTS) - 1
    for c in [final] + list(range(final)):
        sides_y = () if c == final else around[c]
        base = base_of(coef, turned, old, track, sides_y, starts[c], ends[c] - starts[c], base, scale)
    more = (turned, base, like(track.shape, BF16), starts[final], scale)
    out, late = dgate_of(place, new_gate, up, downs, new_pieces, more)
    out = last_of(coef, late, *around[final], out)
    return (fresh[None], out[None])


def solution(mesh):
    return jax.shard_map(
        on_device,
        mesh=mesh,
        in_specs=(
            P("agent", "tp", None),
            P("agent", "tp", None),
            P("agent", None, "tp"),
            P("agent", None, "tp"),
            P("agent", "tp"),
            P("tp", "agent"),
            P(),
            P(),
        ),
        out_specs=(P("agent", None, "tp"), P("agent", None, "tp")),
        check_vma=False,
    )
```

```python
import functools
import math

import jax
import jax.numpy as jnp
from jax import lax
from jax.experimental import pallas as pl
from jax.experimental.pallas import tpu as pltpu
from jax.sharding import PartitionSpec as P


F32 = jnp.float32
BF16 = jnp.bfloat16
PARTS = (2, 8, 4, 2)
VMEM_LIMIT = 67043328


def shifted(value, axis, shift):
    count = lax.axis_size(axis)
    return lax.ppermute(value, axis, [(source, (source + shift) % count) for source in range(count)])


def paired(value, axis):
    return lax.ppermute(value, axis, [(source, source ^ 1) for source in range(lax.axis_size(axis))])


def jumped(value, axis, shift):
    return shifted(value, axis, 2 * shift)


def cost(flops, *arrays):
    return pl.CostEstimate(
        flops=flops, bytes_accessed=sum(a.size * a.dtype.itemsize for a in arrays), transcendentals=0
    )


def block_of(size, most):
    return most if size % most == 0 else size


def column_blocks(width):
    if width % 512 == 0:
        return [0, width // 2, 3 * width // 4, width]
    return [0, width // 2, width] if width % 256 == 0 else [0, width]


def like(shape, dtype):
    return jax.ShapeDtypeStruct(shape, dtype)


def dot(a, b, contract=(1, 0)):
    return lax.dot_general(a, b, (((contract[0],), (contract[1],)), ((), ())), preferred_element_type=F32)


SMEM = pl.BlockSpec(memory_space=pltpu.SMEM)
ANY = pl.BlockSpec(memory_space=pl.ANY)


def call(kernel, **options):
    return pl.pallas_call(kernel, compiler_params=pltpu.CompilerParams(vmem_limit_bytes=VMEM_LIMIT), **options)


def columns(place, i, size):
    return pl.ds(pl.multiple_of(place[i] * size, size), size)


def mixing(place, edge):
    agent, agents = place[0], edge.shape[0]
    right, left = edge[agent], edge[lax.rem(agent + agents - 1, agents)]
    return 1.0 - right - left, right, left


def pack_kernel(*refs):
    *pieces, out_ref, turned_ref = refs
    rows = pieces[0].shape[0]
    for k, ref in enumerate(pieces):
        out_ref[k * rows : (k + 1) * rows, :] = ref[...]
    turned_ref[...] = out_ref[...].T


def pack(pieces):
    rows, width = pieces[0].shape
    rows *= len(pieces)
    dtype = pieces[0].dtype
    return call(pack_kernel, out_shape=[like((rows, width), dtype), like((width, rows), dtype)], name="pack")(
        *pieces
    )


def gate_kernel(scale, tok_ref, w_ref, out_ref):
    out_ref[...] = dot(tok_ref[...], w_ref[...]) * scale


def gate_of(tok, weights, scale):
    rows, depth = tok.shape
    width = weights.shape[1]
    cols = block_of(width, 512)
    out = like((rows, width), F32)
    return call(
        functools.partial(gate_kernel, scale),
        grid=(width // cols,),
        in_specs=[
            pl.BlockSpec((rows, depth), lambda i: (0, 0)),
            pl.BlockSpec((depth, cols), lambda i: (0, i)),
        ],
        out_specs=pl.BlockSpec((rows, cols), lambda i: (0, i)),
        out_shape=out,
        cost_estimate=cost(2 * rows * depth * width, tok, weights, out),
        name="gate",
    )(tok, weights)


def up_kernel(place, tok_ref, *refs):
    total = None
    for i, ref in enumerate(refs[:-1]):
        term = dot(tok_ref[:, columns(place, i, ref.shape[0])], ref[...])
        total = term if total is None else total + term
    refs[-1][...] = total


def up_of(place, tok, pieces):
    depth, width = pieces[0].shape
    rows = tok.shape[0]
    cols = block_of(width, 256)
    out = like((rows, width), F32)
    return call(
        up_kernel,
        grid=(width // cols,),
        in_specs=[SMEM, pl.BlockSpec(tok.shape, lambda n: (0, 0))]
        + [pl.BlockSpec((depth, cols), lambda n: (0, n))] * len(pieces),
        out_specs=pl.BlockSpec((rows, cols), lambda n: (0, n)),
        out_shape=out,
        cost_estimate=cost(2 * rows * depth * width * len(pieces), tok, out, *pieces),
        name="up",
    )(place, tok, *pieces)


def add_share(place, gate, up_ref, weights, carry, bring, outs, total):
    hidden = (jax.nn.sigmoid(gate) * gate * up_ref[...]).astype(BF16)
    n, last = pl.program_id(0), pl.num_programs(0) - 1
    if bring is not None:

        @pl.when(n == 0)
        def _():
            bring.wait()

    for i, ref in enumerate(weights):
        term = dot(hidden, ref[...])
        if bring is not None:
            total[i] += term
            continue

        @pl.when(n == 0)
        def _():
            total[i] = term if carry is None else carry[i] + term

        @pl.when(n > 0)
        def _():
            total[i] += term

    if not outs:
        return

    @pl.when(n == last)
    def _():
        cols = weights[0].shape[1]
        for i in range(len(weights)):
            start = 0
            for ref in outs:
                stop = start + ref.shape[0]
                ref[:, columns(place, i, cols)] = total[i, start:stop, :].astype(BF16)
                start = stop


def share_kernel(count, place, gate_ref, up_ref, *refs):
    add_share(place, gate_ref[...], up_ref, refs[:count], None, None, refs[count:-1], refs[-1])


def share_outs(rows, depth, pairs):
    near, piece = rows // 2, rows // 2 // pairs
    outs = [like((near, depth), BF16)] + [like((piece, depth), BF16)] * pairs
    return outs, [pl.BlockSpec(o.shape, lambda n: (0, 0)) for o in outs]


def share_of(place, gate, up, downs, pairs):
    rows, width = gate.shape
    cols = downs[0].shape[1]
    depth = cols * len(downs)
    block = block_of(width, 256)
    spec = pl.BlockSpec((rows, block), lambda n: (0, n))
    outs, out_specs = share_outs(rows, depth, pairs)
    return call(
        functools.partial(share_kernel, len(downs)),
        grid=(width // block,),
        in_specs=[SMEM, spec, spec] + [pl.BlockSpec((block, cols), lambda n: (n, 0))] * len(downs),
        out_specs=out_specs,
        out_shape=outs,
        scratch_shapes=[pltpu.VMEM((len(downs), rows, cols), F32)],
        cost_estimate=cost(2 * rows * width * depth, gate, up, *downs, *outs),
        name="share",
    )(place, gate, up, *downs)


def fresh_kernel(count, scale, first, last, place, edge, size, tok_ref, p_ref, left_ref, right_ref, t_ref, up_ref, *refs):
    weights, refs = refs[:count], refs[count:]
    carry = bring = None
    if not first:
        carry, refs = refs[0], refs[3:]
    if carry is not None and last:
        bring, refs = pltpu.make_async_copy(carry, refs[-2], refs[-1]), refs[:-1]

        @pl.when(pl.program_id(0) == 0)
        def _():
            bring.start()

    fresh_ref, gate_ref, *refs = refs
    own, e_right, e_left = mixing(place, edge)
    mixed = (
        own * p_ref[...].astype(F32)
        + e_right * right_ref[...].astype(F32)
        + e_left * left_ref[...].astype(F32)
    )
    fresh = (mixed - size[0] * t_ref[...].astype(F32)).astype(BF16)
    fresh_ref[...] = fresh
    gate = dot(tok_ref[...], fresh) * scale
    gate_ref[...] = gate
    add_share(place, gate, up_ref, weights, carry, bring, refs[:-1], refs[-1])


def fresh_of(place, edge, size, tok, param, left, right, track, up, downs, pairs, scale, start, so_far):
    depth, width = param.shape
    rows, part = tok.shape[0], left.shape[1]
    cols = downs[0].shape[1]
    block = math.gcd(256, start, part)
    base = start // block
    first, last = so_far is None, start + part == width
    there = pl.BlockSpec((depth, block), lambda n: (0, base + n))
    here = pl.BlockSpec((depth, block), lambda n: (0, n))
    hidden = pl.BlockSpec((rows, block), lambda n: (0, base + n))
    operands = [place, edge, size, tok, param, left, right, track, up, *downs]
    specs = [SMEM, SMEM, SMEM, pl.BlockSpec(tok.shape, lambda n: (0, 0)), there, here, here, there, hidden]
    specs += [pl.BlockSpec((block, cols), lambda n: (base + n, 0))] * len(downs)
    total = (len(downs), rows, cols)
    whole = pl.BlockSpec(total, lambda n: (0, 0, 0))
    aliases = {}
    if not first:
        aliases = {len(operands) + 1: 0, len(operands) + 2: 1}
        operands += [so_far[2], so_far[0], so_far[1]]
        specs += [ANY if last else whole, ANY, ANY]
    outs, out_specs = [like((depth, width), BF16), like((rows, width), F32)], [there, hidden]
    scratch = []
    if last:
        more, more_specs = share_outs(rows, cols * len(downs), pairs)
        outs, out_specs = outs + more, out_specs + more_specs
        scratch = [pltpu.VMEM(total, F32)] + ([] if first else [pltpu.SemaphoreType.DMA(())])
    else:
        outs, out_specs = outs + [like(total, F32)], out_specs + [whole]
    return call(
        functools.partial(fresh_kernel, len(downs), scale, first, last),
        grid=(part // block,),
        in_specs=specs,
        out_specs=out_specs,
        out_shape=outs,
        scratch_shapes=scratch,
        input_output_aliases=aliases,
        cost_estimate=cost(4 * rows * depth * part, left, left, right, right, left, up, *downs),
        name="fresh",
    )(*operands)


def join_kernel(mine_ref, other_ref, out_ref):
    out_ref[...] = (mine_ref[...].astype(F32) + other_ref[...].astype(F32)).astype(BF16)


def join(near, other, j):
    out = like(other.shape, BF16)
    whole = pl.BlockSpec(other.shape, lambda i: (0, 0))
    return call(
        join_kernel,
        grid=(1,),
        in_specs=[pl.BlockSpec(other.shape, lambda i: (j, 0)), whole],
        out_specs=whole,
        out_shape=out,
        cost_estimate=cost(out.size, other, other, out),
        name="join",
    )(near, other)


def err_kernel(near_ref, target_ref, *refs):
    total = near_ref[...].astype(F32)
    for ref in refs[:-1]:
        total = total + ref[...].astype(F32)
    refs[-1][...] = (2.0 * (total - target_ref[...].astype(F32))).astype(BF16)


def err_of(near, targets, others):
    whole = pl.BlockSpec(targets.shape, lambda i: (0, 0))
    return call(
        err_kernel,
        grid=(1,),
        in_specs=[whole] * (2 + len(others)),
        out_specs=whole,
        out_shape=like(targets.shape, BF16),
        cost_estimate=cost(targets.size * 4, targets, targets, targets, *others),
        name="err",
    )(near, targets, *others)


def dgate_block(count, place, gate_ref, up_ref, refs, err):
    weights, pieces = refs[:count], refs[count:]

    @pl.when(pl.program_id(0) == 0)
    def _():
        rows = pieces[0].shape[0]
        for k, ref in enumerate(pieces):
            err[k * rows : (k + 1) * rows, :] = ref[...]

    back = None
    for i, ref in enumerate(weights):
        term = dot(err[:, columns(place, i, ref.shape[1])], ref[...], (1, 1))
        back = term if back is None else back + term
    gate = gate_ref[...]
    sig = jax.nn.sigmoid(gate)
    return (back * up_ref[...] * sig * (1.0 + gate * (1.0 - sig))).astype(BF16)


def dgate_kernel(count, place, gate_ref, up_ref, *refs):
    refs[-2][...] = dgate_block(count, place, gate_ref, up_ref, refs[:-2], refs[-1])


def tail_kernel(count, scale, place, turned_hbm, base_ref, gate_ref, up_ref, *refs):
    *refs, out_ref, late_ref, err, turned, turned_sem = refs
    bring_turned = pltpu.make_async_copy(turned_hbm, turned, turned_sem)
    first = pl.program_id(0) == 0

    @pl.when(first)
    def _():
        bring_turned.start()

    value = dgate_block(count, place, gate_ref, up_ref, refs, err)

    @pl.when(first)
    def _():
        bring_turned.wait()

    rows = out_ref.shape[0]
    total = base_ref[...] + dot(turned[...], value) * scale
    out_ref[...] = total[:rows].astype(BF16)
    late_ref[...] = total[rows:]


def dgate_of(place, gate, up, downs, pieces, more=None):
    width, cols = downs[0].shape
    rows = gate.shape[0]
    block = block_of(width, 512)
    hidden = pl.BlockSpec((rows, block), lambda n: (0, n))
    whole = pl.BlockSpec(pieces[0].shape, lambda n: (0, 0))
    depth = cols * len(downs)
    operands, specs, scratch = [place], [SMEM], [pltpu.VMEM((rows, depth), BF16)]
    outs, out_specs = [like((rows, width), BF16)], [hidden]
    kernel, flops = functools.partial(dgate_kernel, len(downs)), 2 * rows * width * depth
    if more is not None:
        turned, base, out, done, scale = more
        tall = base.shape[0]
        operands += [turned, base]
        specs += [ANY, pl.BlockSpec((tall, block), lambda n: (0, n))]
        scratch += [pltpu.VMEM(turned.shape, turned.dtype), pltpu.SemaphoreType.DMA(())]
        outs = [out, like((tall - done, width), F32)]
        out_specs = [pl.BlockSpec((size, block), lambda n: (0, n)) for size in (done, tall - done)]
        kernel, flops = functools.partial(tail_kernel, len(downs), scale), 2 * flops
    return call(
        kernel,
        grid=(width // block,),
        in_specs=specs
        + [hidden, hidden]
        + [pl.BlockSpec((block, cols), lambda n: (n, 0))] * len(downs)
        + [whole] * len(pieces),
        out_specs=out_specs,
        out_shape=outs,
        scratch_shapes=scratch,
        cost_estimate=cost(flops, gate, up, *outs, *downs, *pieces),
        name="dgate",
    )(*operands, gate, up, *downs, *pieces)


def base_kernel(scale, place, edge, turned_ref, old_ref, t_ref, *rest):
    own, e_right, e_left = mixing(place, edge)
    mixed = own * t_ref[...].astype(F32)
    if len(rest) > 2:
        mixed = mixed + e_right * rest[1][...].astype(F32) + e_left * rest[0][...].astype(F32)
    rest[-1][...] = mixed - dot(turned_ref[...], old_ref[...]) * scale


def base_of(place, edge, turned, old, track, sides, start, part, so_far, scale):
    depth, width = track.shape
    rows = turned.shape[1]
    step = math.gcd(256, start, part)
    base = start // step
    there = pl.BlockSpec((step, width), lambda k: (base + k, 0))
    here = pl.BlockSpec((step, width), lambda k: (k, 0))
    operands = [place, edge, turned, old, track, *sides]
    specs = [SMEM, SMEM, pl.BlockSpec((step, rows), lambda k: (base + k, 0))]
    specs += [pl.BlockSpec((rows, width), lambda k: (0, 0)), there] + [here] * len(sides)
    aliases = {}
    if so_far is not None:
        aliases = {len(operands): 0}
        operands.append(so_far)
        specs.append(ANY)
    return call(
        functools.partial(base_kernel, scale),
        grid=(part // step,),
        in_specs=specs,
        out_specs=there,
        out_shape=like((depth, width), F32),
        input_output_aliases=aliases,
        cost_estimate=cost(2 * rows * part * width, like((part, width), F32), old, *sides),
        name="base",
    )(*operands)


def last_kernel(place, edge, late_ref, left_ref, right_ref, so_far, out_ref):
    _, e_right, e_left = mixing(place, edge)
    mixed = e_right * right_ref[...].astype(F32) + e_left * left_ref[...].astype(F32)
    out_ref[...] = (late_ref[...] + mixed).astype(BF16)


def last_of(place, edge, late, left, right, out):
    part, width = late.shape
    start = out.shape[0] - part
    step = math.gcd(128, start, part)
    base = start // step
    here = pl.BlockSpec((step, width), lambda k: (k, 0))
    return call(
        last_kernel,
        grid=(part // step,),
        in_specs=[SMEM, SMEM, here, here, here, ANY],
        out_specs=pl.BlockSpec((step, width), lambda k: (base + k, 0)),
        out_shape=like(out.shape, BF16),
        input_output_aliases={5: 0},
        cost_estimate=cost(late.size, late, left, right, left),
        name="last",
    )(place, edge, late, left, right, out)


def spread(piece, axis, pairs):
    near = [piece] + [jumped(piece, axis, j) for j in range(1, pairs)]
    return near + [paired(part, axis) for part in near]


def on_device(tokens, targets, params, tracker, up_weight, down_weight, edge_weight, step_size):
    token_rows, target_rows, param, track = tokens[0], targets[0], params[0], tracker[0]
    agents, count = lax.axis_size("agent"), lax.axis_size("tp")
    half, pairs = agents // 2, count // 2
    depth = param.shape[0]
    scale = 1.0 / depth**0.5

    index = lax.axis_index("agent")
    even, parity = index // 2, index % 2
    chips = [lax.rem(even - j + half, half) for j in range(half)]
    place = jnp.stack([2 * c + parity for c in chips] + [2 * c + 1 - parity for c in chips]).astype(jnp.int32)

    def gathered(weight):
        own = [weight] + [jumped(weight, "agent", j) for j in range(1, half)]
        return own + [paired(w, "agent") for w in own]

    ups, downs = gathered(up_weight), gathered(down_weight)
    edges = column_blocks(param.shape[1])
    blocks = len(edges) - 1
    sides = []
    for start, end in zip(edges, edges[1:]):
        p = param[:, start:end]
        sides.append((shifted(p, "agent", 1), shifted(p, "agent", -1)))
    ends = [depth * sum(PARTS[: c + 1]) // sum(PARTS) for c in range(len(PARTS))]
    starts = [0] + ends[:-1]
    around = []
    for start, end in zip(starts, ends):
        t = track[start:end]
        around.append((shifted(t, "agent", 1), shifted(t, "agent", -1)))

    tok, turned = pack(spread(token_rows, "tp", pairs))
    gate = gate_of(tok, param, scale)
    up = up_of(place, tok, ups)

    def errors(shares):
        near, *far = shares
        order = list(range(1, pairs)) + [0]
        sent = {j: paired(far[j], "tp") for j in order}
        summed = []
        for j in order[:-1]:
            value = join(near, sent[j], j)
            summed.append(jumped(value, "tp", -j))
        err = err_of(near, target_rows, [sent[0], *summed])
        return spread(err, "tp", pairs)

    shares = share_of(place, gate, up, downs, pairs)
    made = None
    for h in range(blocks - 1):
        made = fresh_of(
            place, edge_weight, step_size, tok, param, *sides[h], track, up, downs, pairs, scale, edges[h], made
        )
    old_pieces = errors(shares)
    later, old_pieces[0] = lax.optimization_barrier((step_size, old_pieces[0]))
    fresh, new_gate, *shares = fresh_of(
        place, edge_weight, later, tok, param, *sides[-1], track, up, downs, pairs, scale, edges[-2], made
    )
    new_pieces = errors(shares)
    (old,) = dgate_of(place, gate, up, downs, old_pieces)
    base = None
    final = len(PARTS) - 1
    for c in [final] + list(range(final)):
        sides_y = () if c == final else around[c]
        base = base_of(place, edge_weight, turned, old, track, sides_y, starts[c], ends[c] - starts[c], base, scale)
    more = (turned, base, like(track.shape, BF16), starts[final], scale)
    out, late = dgate_of(place, new_gate, up, downs, new_pieces, more)
    out = last_of(place, edge_weight, late, *around[final], out)
    return (fresh[None], out[None])


def solution(mesh):
    return jax.shard_map(
        on_device,
        mesh=mesh,
        in_specs=(
            P("agent", "tp", None),
            P("agent", "tp", None),
            P("agent", None, "tp"),
            P("agent", None, "tp"),
            P("agent", "tp"),
            P("tp", "agent"),
            P(),
            P(),
        ),
        out_specs=(P("agent", None, "tp"), P("agent", None, "tp")),
        check_vma=False,
    )
```
